32 devices in a mesh: groups: 2 (over y), ctx: 4 (over z), head: 4 (over x, core).
Axes of the slice: x: 2, y: 2, z: 4, core: 2. Of those that a mesh axis runs over, the one named last changes fastest.
Arguments:
- query: bfloat16 [8, 64, 32, 128], P('groups', 'head'), parts along dimension 0
- key_cache: bfloat16 [8, 8192, 8, 128], P('groups', 'ctx', 'head'), parts along dimension 0
- value_cache: bfloat16 [8, 8192, 8, 128], P('groups', 'ctx', 'head'), parts along dimension 0, may hold values from -6 to 6
- new_key: bfloat16 [8, 8, 32, 128], P('groups', 'head'), parts along dimension 0, may hold values from -9 to 9
- new_value: bfloat16 [8, 8, 32, 128], P('groups', 'head'), parts along dimension 0, may hold values from -6 to 6
- lengths: int32 [8], P('groups'), parts along dimension 0, may hold values from 256 to 8192, as said below
- out_weight: bfloat16 [8192, 8192], P('head', 'ctx'), may hold values from -0.0625 to 0.0625
Outputs:
- projected: float32 [8, 32, 8192], P('groups', None, 'ctx'), parts along dimension 0
The draws below stay inside these ranges and needn't reach their ends.
There are 2 independent parts, one for each index of `groups`. The reference program is written for one: setup_inputs(seed, part) draws one part's arguments, and reference() takes and returns one part's arrays. A program takes and returns all parts, laid end to end along the dimension named above; an argument that names none is the same for every part. Nothing has to cross between parts.
Inputs may be any that keep to these rules, and one draw needn't show every extreme that they name: `lengths`: multiples of 256; in every draw exactly one sequence has length 8192, the others less.
All inputs are finite; a program needn't handle non-finite values.
Results may differ from the reference program's by a relative error of at most 0.003.
Values sent between devices are 32-bit elements; how exact they have to be, the bound alone decides.
A program may use at most 128 MiB of HBM per device.

```python
import math
import jax
import jax.numpy as jnp
from jax import lax

QH = 64
KVH = 8
HD = 128
D = 8192
SEQS = 4
CTX_DEV = 2048
DRAFT = 32
BLOCK = 256
CTX = 8192
N_CTX = 4


def plant_table(key):
    group_size = QH // KVH
    planted = jax.random.normal(jax.random.fold_in(key, 11), (SEQS, 2 * group_size, KVH, HD), jnp.float32)
    return planted


def draw_key_cache(key, part):
    group_size = QH // KVH
    planted = plant_table(key)
    remainder = jax.random.normal(jax.random.fold_in(key, 12), (SEQS, CTX - 2 * group_size, KVH, HD), jnp.float32)
    return jnp.concatenate((planted, remainder), axis=1).astype(jnp.bfloat16)


def draw_query(key, part):
    baseline = 3.0 * jnp.clip(jax.random.normal(jax.random.fold_in(key, 21), (SEQS, QH, DRAFT, HD), jnp.float32), -6.0, 6.0)
    return baseline.astype(jnp.bfloat16)


def draw_lengths(key, part):
    block_count = CTX // BLOCK
    picked = jax.random.randint(jax.random.fold_in(key, 1), (SEQS,), 1, block_count)
    full_seq = jax.random.randint(jax.random.fold_in(key, 2), (), 0, SEQS)
    picked = jnp.where(jnp.arange(SEQS) == full_seq, block_count, picked)
    return (picked * BLOCK).astype(jnp.int32)


def level_of(stream_key, extent, pieces, smallest, high):
    level = 1.0
    for axis_at, parts in pieces:
        heights = jax.random.uniform(jax.random.fold_in(jax.random.fold_in(stream_key, 6), axis_at), (parts,), jnp.float32, smallest / len(pieces), high / len(pieces))
        level = level * jnp.repeat(jnp.exp(heights), extent[axis_at] // parts).reshape((-1,) + (1,) * (len(extent) - 1 - axis_at))
    return level


def normal_values(key, dims, width, reach, split=(), kind=jnp.bfloat16):
    result = width * jax.random.normal(key, dims, jnp.float32)
    if split:
        result = result * level_of(key, dims, split, -0.22, 0.18)
    return jnp.clip(result, -reach, reach).astype(kind)


def setup_inputs(seed: int = 0, part: int = 0) -> dict:
    splits = jax.random.split(jax.random.key(seed), 8)
    part_keys = jax.random.split(jax.random.fold_in(splits[7], part), 8)
    query = draw_query(jax.random.fold_in(jax.random.fold_in(splits[7], part), 71), part)
    key_cache = draw_key_cache(jax.random.fold_in(jax.random.fold_in(splits[7], part), 71), part)
    value_cache = normal_values(part_keys[2], (SEQS, CTX, KVH, HD), 1.0, 6.0, ((1, 4), (2, 4)))
    new_key = normal_values(part_keys[3], (SEQS, KVH, DRAFT, HD), 1.5, 9.0, ((1, 4),))
    new_value = normal_values(part_keys[4], (SEQS, KVH, DRAFT, HD), 1.0, 6.0, ((1, 4),))
    lengths = draw_lengths(jax.random.fold_in(jax.random.fold_in(splits[7], part), 71), part)
    out_weight = normal_values(splits[6], (QH * HD, D), (QH * HD) ** -0.5, 0.0625, ((0, 4), (1, 4)))
    return dict(query=query, key_cache=key_cache, value_cache=value_cache, new_key=new_key, new_value=new_value, lengths=lengths, out_weight=out_weight)


very_low = -1e+30

def reference(query, key_cache, value_cache, new_key, new_value, lengths, out_weight):
    seq_count, q_count, draft_len, head_dim = query.shape
    kv_count = key_cache.shape[2]
    group_rows = q_count // kv_count * draft_len
    scaling = 1.0 / math.sqrt(head_dim)
    grouped = query.reshape(seq_count, kv_count, group_rows, head_dim).astype(jnp.float32)

    def block_stats(block_index):
        offset = (block_index * CTX_DEV).astype(jnp.int32)
        key_block = lax.dynamic_slice_in_dim(key_cache, offset, CTX_DEV, 1).astype(jnp.float32)
        value_block = lax.dynamic_slice_in_dim(value_cache, offset, CTX_DEV, 1).astype(jnp.float32)
        scores = jnp.einsum('sgrd,stgd->sgrt', grouped, key_block) * scaling
        position = offset + jnp.arange(CTX_DEV, dtype=jnp.int32)
        usable = (position[None, :] < lengths[:, None])[:, None, None, :]
        masked = jnp.where(usable, scores, very_low)
        block_top = lax.optimization_barrier(jnp.max(masked, axis=-1))
        weights = jnp.where(usable, jnp.exp(masked - block_top[..., None]), 0.0).astype(jnp.bfloat16)
        widened = weights.astype(jnp.float32)
        return (block_top, lax.optimization_barrier(jnp.sum(widened, axis=-1)), jnp.einsum('sgrt,stgd->sgrd', widened, value_block))
    tops, sums_all, numer_all = lax.map(block_stats, jnp.arange(N_CTX, dtype=jnp.int32))
    global_top = lax.optimization_barrier(jnp.max(tops, axis=0))
    factor = jnp.exp(tops - global_top)
    totals = lax.optimization_barrier(jnp.sum(sums_all * factor, axis=0))
    numerators = lax.optimization_barrier(jnp.sum(numer_all * factor[..., None], axis=0))
    own_scores = jnp.einsum('sgrd,sgjd->sgrj', grouped, new_key.astype(jnp.float32)) * scaling
    row_index = jnp.arange(group_rows) % draft_len
    causal = jnp.arange(draft_len)[None, :] <= row_index[:, None]
    own_scores = jnp.where(causal, own_scores, very_low)
    overall = jnp.maximum(global_top, lax.optimization_barrier(jnp.max(own_scores, axis=-1)))
    carried = jnp.exp(global_top - overall)
    fresh_weights = jnp.where(causal, jnp.exp(own_scores - overall[..., None]), 0.0)
    denominator = totals * carried + lax.optimization_barrier(jnp.sum(fresh_weights, axis=-1))
    numerators = numerators * carried[..., None] + jnp.einsum('sgrj,sgjd->sgrd', fresh_weights, new_value.astype(jnp.float32))
    attended = (numerators / denominator[..., None]).reshape(seq_count, q_count, draft_len, head_dim)
    attended = jnp.transpose(attended, (0, 2, 1, 3)).reshape(seq_count * draft_len, q_count * head_dim).astype(jnp.bfloat16)
    projected = jnp.dot(attended, out_weight, preferred_element_type=jnp.float32)
    return projected.reshape(seq_count, draft_len, -1)
```

```python
import functools
import math

import jax
import jax.numpy as jnp
from jax import lax
from jax.experimental import pallas as pl
from jax.experimental.pallas import tpu as pltpu
from jax.sharding import PartitionSpec as P

very_low = -1e30
MESH = pl.DeviceIdType.MESH
LANES = 128
PAGE = 256


def plain_shards(query, key_cache, value_cache, new_key, new_value, lengths, out_weight):
    seq_count, q_count, draft_len, head_dim = query.shape
    ctx_len = key_cache.shape[1]
    kv_count = key_cache.shape[2]
    group_rows = q_count // kv_count * draft_len
    scaling = 1.0 / math.sqrt(head_dim)
    grouped = query.reshape(seq_count, kv_count, group_rows, head_dim)
    scores = (
        jnp.einsum("sgrd,stgd->sgrt", grouped, key_cache, preferred_element_type=jnp.float32)
        * scaling
    )
    position = lax.axis_index("ctx") * ctx_len + jnp.arange(ctx_len, dtype=jnp.int32)
    usable = (position[None, :] < lengths[:, None])[:, None, None, :]
    masked = jnp.where(usable, scores, very_low)
    block_top = jnp.max(masked, axis=-1)
    weights = jnp.where(usable, jnp.exp(masked - block_top[..., None]), 0.0).astype(jnp.bfloat16)
    totals = jnp.sum(weights.astype(jnp.float32), axis=-1)
    numerators = jnp.einsum(
        "sgrt,stgd->sgrd", weights, value_cache, preferred_element_type=jnp.float32
    )
    global_top = lax.pmax(block_top, "ctx")
    factor = jnp.exp(block_top - global_top)
    totals, numerators = lax.psum((totals * factor, numerators * factor[..., None]), "ctx")
    own_scores = (
        jnp.einsum("sgrd,sgjd->sgrj", grouped, new_key, preferred_element_type=jnp.float32)
        * scaling
    )
    row_index = jnp.arange(group_rows) % draft_len
    causal = jnp.arange(draft_len)[None, :] <= row_index[:, None]
    own_scores = jnp.where(causal, own_scores, very_low)
    overall = jnp.maximum(global_top, jnp.max(own_scores, axis=-1))
    carried = jnp.exp(global_top - overall)
    fresh_weights = jnp.where(causal, jnp.exp(own_scores - overall[..., None]), 0.0)
    denominator = totals * carried + jnp.sum(fresh_weights, axis=-1)
    numerators = numerators * carried[..., None] + jnp.einsum(
        "sgrj,sgjd->sgrd", fresh_weights, new_value.astype(jnp.float32)
    )
    attended = (numerators / denominator[..., None]).reshape(
        seq_count, q_count, draft_len, head_dim
    )
    attended = (
        jnp.transpose(attended, (0, 2, 1, 3))
        .reshape(seq_count * draft_len, q_count * head_dim)
        .astype(jnp.bfloat16)
    )
    partial_out = jnp.dot(attended, out_weight, preferred_element_type=jnp.float32).reshape(
        seq_count, draft_len, -1
    )
    return lax.psum(partial_out, "head")


def column(values, at):
    return values[:, at : at + 1]


def kernel(
    n, draft, chunk,
    q_ref, k_hbm, v_hbm, nk_ref, nv_ref, len_ref, w_hbm, out_ref,
    kbuf, vbuf, wbuf, sbuf, acc, msg, rmsg, ag, send_a, keep, recv_a, send_b, recv_b,
    ksem, vsem, wsem, rs_send, rs_recv, ag_send, ag_recv,
    a_send, a_recv, b_send, b_recv, c_send, c_recv,
):
    me = lax.axis_index("ctx")
    head = lax.axis_index("head")
    side = lax.rem(head, 2)
    other = 1 - side
    pair = head - side + other
    upper = lax.rem(lax.div(head, 2), 2)
    across = head + 2 - 4 * upper
    rows = q_ref.shape[1] // 2
    span = kbuf.shape[1]
    half = wbuf.shape[2]
    steps = span // chunk
    scale = math.log2(math.e) / math.sqrt(q_ref.shape[2])
    order = [k for k in (1, n - 1) + tuple(range(2, n - 1))]

    def seq_at(offset):
        return lax.rem(me + offset, n)

    barrier = pltpu.get_barrier_semaphore()
    for offset in range(1, n):
        pl.semaphore_signal(barrier, inc=1, device_id={"ctx": seq_at(offset)}, device_id_type=MESH)
    pl.semaphore_signal(barrier, inc=1, device_id={"head": pair}, device_id_type=MESH)
    pl.semaphore_signal(barrier, inc=1, device_id={"head": across}, device_id_type=MESH)

    def k_copy(offset):
        s = seq_at(offset)
        return pltpu.make_async_copy(k_hbm.at[s], kbuf.at[offset], ksem.at[offset])

    def v_copy(offset):
        s = seq_at(offset)
        return pltpu.make_async_copy(v_hbm.at[s], vbuf.at[offset], vsem.at[offset])

    def w_copy(i):
        return pltpu.make_async_copy(w_hbm.at[:, pl.ds(i * half, half)], wbuf.at[i], wsem.at[i])

    for offset in order + [0]:
        k_copy(offset).start()
        v_copy(offset).start()
    w_copy(0).start()
    w_copy(1).start()

    lane = lax.broadcasted_iota(jnp.int32, (rows, LANES), 1)
    even_lane = lax.rem(lane, 2) == 0
    sub = lax.broadcasted_iota(jnp.int32, (1, 16, LANES), 1)
    even_row = jnp.where(lax.rem(sub, 2) == 0, 1.0, 0.0).astype(jnp.bfloat16)
    odd_row = jnp.where(lax.rem(sub, 2) == 0, 0.0, 1.0).astype(jnp.bfloat16)

    def spread(block):
        tiles = block.reshape(chunk // 16, 16, LANES)
        return jnp.concatenate(
            [(tiles * even_row).reshape(chunk, LANES), (tiles * odd_row).reshape(chunk, LANES)],
            axis=1,
        )

    def attend(offset):
        s = seq_at(offset)
        grouped = jnp.concatenate([q_ref[s, :rows], q_ref[s, rows:]], axis=1)
        usable = len_ref[s] - me * (span // 2)
        k_copy(offset).wait()
        per = 2 * PAGE

        def bias(j, page):
            return jnp.where((j * (chunk // per) + page) * PAGE < usable, 0.0, -very_low)

        def score(j, top):
            at = pl.multiple_of(j * chunk, chunk)
            keys = spread(kbuf[offset, pl.ds(at, chunk), :])
            scores = lax.dot_general(
                grouped, keys, (((1,), (1,)), ((), ())), preferred_element_type=jnp.float32
            )
            sbuf[j] = scores
            for page in range(chunk // per):
                tiles = [
                    scores[:, page * per + i * LANES : page * per + (i + 1) * LANES]
                    for i in range(per // LANES)
                ]
                top = jnp.maximum(top, functools.reduce(jnp.maximum, tiles) - bias(j, page))
            return top

        top = lax.fori_loop(0, steps, score, jnp.full((rows, LANES), very_low, jnp.float32))
        tops = [
            jnp.max(jnp.where(even_lane, top, very_low), axis=1, keepdims=True) * scale,
            jnp.max(jnp.where(even_lane, very_low, top), axis=1, keepdims=True) * scale,
        ]
        shift = jnp.where(even_lane, tops[0], tops[1])
        v_copy(offset).wait()
        acc[...] = jnp.zeros_like(acc)

        def weigh(j, total):
            at = pl.multiple_of(j * chunk, chunk)
            pieces = []
            for page in range(chunk // per):
                shifted = shift + bias(j, page)
                for i in range(per // LANES):
                    piece = jnp.exp2(
                        sbuf[j, :, page * per + i * LANES : page * per + (i + 1) * LANES] * scale
                        - shifted
                    )
                    total = total + piece
                    pieces.append(piece.astype(jnp.bfloat16))
            weights = jnp.concatenate(pieces, axis=1)
            values = spread(vbuf[offset, pl.ds(at, chunk), :])
            acc[...] += jnp.dot(weights, values, preferred_element_type=jnp.float32)
            return total

        total = lax.fori_loop(0, steps, weigh, jnp.zeros((rows, LANES), jnp.float32))
        sums = [
            jnp.sum(jnp.where(even_lane, total, 0.0), axis=1, keepdims=True),
            jnp.sum(jnp.where(even_lane, 0.0, total), axis=1, keepdims=True),
        ]
        return tops, sums

    def send_partial(offset):
        return pltpu.make_async_remote_copy(
            src_ref=msg.at[offset - 1], dst_ref=rmsg.at[offset - 1],
            send_sem=rs_send.at[offset - 1], recv_sem=rs_recv.at[offset - 1],
            device_id={"ctx": seq_at(offset)}, device_id_type=MESH,
        )

    for index, offset in enumerate(order):
        tops, sums = attend(offset)
        slot = offset - 1
        msg[slot, :rows, :] = acc[:, :LANES]
        msg[slot, rows : 2 * rows, :] = acc[:, LANES:]
        stats = jnp.where(
            lane == 0, tops[0],
            jnp.where(lane == 1, sums[0], jnp.where(lane == 2, tops[1], sums[1])),
        ).T
        for i in range(rows // LANES):
            msg[slot, 2 * rows + 8 * i : 2 * rows + 8 * (i + 1), :] = stats[
                :8, i * LANES : (i + 1) * LANES
            ]
        if index == 0:
            pl.semaphore_wait(barrier, n + 1)
        send_partial(offset).start()

    tops, sums = attend(0)
    row_in = lax.rem(lax.broadcasted_iota(jnp.int32, (rows, draft), 0), draft)
    causal = lax.broadcasted_iota(jnp.int32, (rows, draft), 1) <= row_in
    own = []
    for g in range(2):
        fresh = lax.dot_general(
            q_ref[me, g * rows : (g + 1) * rows], nk_ref[me, g],
            (((1,), (1,)), ((), ())), preferred_element_type=jnp.float32,
        ) * scale
        fresh = jnp.where(causal, fresh, very_low)
        own.append((fresh, jnp.max(fresh, axis=1, keepdims=True)))

    stats = []
    for offset in order:
        send_partial(offset).wait_recv()
        slot = offset - 1
        packed = jnp.concatenate(
            [rmsg[slot, 2 * rows + 8 * i : 2 * rows + 8 * (i + 1), :] for i in range(rows // LANES)],
            axis=1,
        )
        packed = jnp.concatenate([packed, jnp.zeros((LANES - 8, rows), jnp.float32)], axis=0)
        stats.append((slot, packed.T))

    for g in range(2):
        fresh, fresh_top = own[g]
        overall = jnp.maximum(tops[g], fresh_top)
        for slot, values in stats:
            overall = jnp.maximum(overall, column(values, 2 * g))
        fresh = jnp.where(causal, jnp.exp2(fresh - overall), 0.0)
        carried = jnp.exp2(tops[g] - overall)
        denominator = jnp.sum(fresh, axis=1, keepdims=True) + sums[g] * carried
        numerator = acc[:, g * LANES : (g + 1) * LANES] * carried + jnp.dot(
            fresh.astype(jnp.bfloat16), nv_ref[me, g], preferred_element_type=jnp.float32
        )
        for slot, values in stats:
            carried = jnp.exp2(column(values, 2 * g) - overall)
            denominator = denominator + column(values, 2 * g + 1) * carried
            numerator = numerator + rmsg[slot, g * rows : (g + 1) * rows, :] * carried
        ag[0, g * rows : (g + 1) * rows, :] = numerator / denominator

    def send_attended(offset):
        return pltpu.make_async_remote_copy(
            src_ref=ag.at[0], dst_ref=ag.at[offset],
            send_sem=ag_send.at[offset - 1], recv_sem=ag_recv.at[offset - 1],
            device_id={"ctx": seq_at(offset)}, device_id_type=MESH,
        )

    for offset in order:
        send_attended(offset).start()

    def swap_a(slot):
        return pltpu.make_async_remote_copy(
            src_ref=send_a.at[slot], dst_ref=recv_a.at[slot],
            send_sem=a_send.at[slot], recv_sem=a_recv.at[slot],
            device_id={"head": pair}, device_id_type=MESH,
        )

    def swap_b(slot):
        return pltpu.make_async_remote_copy(
            src_ref=send_b.at[slot], dst_ref=recv_b.at[slot],
            send_sem=b_send.at[slot], recv_sem=b_recv.at[slot],
            device_id={"head": across}, device_id_type=MESH,
        )

    def swap_c(slot):
        s = seq_at(n - slot)
        return pltpu.make_async_remote_copy(
            src_ref=out_ref.at[side, s], dst_ref=out_ref.at[side, s],
            send_sem=c_send.at[slot], recv_sem=c_recv.at[slot],
            device_id={"head": pair}, device_id_type=MESH,
        )

    wide = 2 * LANES

    def project(slot):
        heads = ag.shape[1] // draft
        attended = jnp.concatenate(
            [ag[slot, h * draft : (h + 1) * draft, :].astype(jnp.bfloat16) for h in range(heads)],
            axis=1,
        )
        for target, which in ((send_a, other), (keep, side)):
            @pl.loop(0, half // wide)
            def _(i):
                at = pl.ds(pl.multiple_of(i * wide, wide), wide)
                target[slot, :, at] = jnp.dot(
                    attended, wbuf[which, :, at], preferred_element_type=jnp.float32
                )
            if target is send_a:
                swap_a(slot).start()

    def join_pair(slot):
        swap_a(slot).wait_recv()
        send_b[slot] = keep[slot] + recv_a[slot]
        swap_b(slot).start()

    def join_across(slot):
        swap_b(slot).wait_recv()
        out_ref[side, seq_at(n - slot)] = send_b[slot] + recv_b[slot]
        swap_c(slot).start()

    w_copy(0).wait()
    w_copy(1).wait()
    slots = [0] + order
    for i in range(n + 2):
        if i < n:
            if slots[i]:
                send_attended(slots[i]).wait_recv()
            project(slots[i])
        if 0 <= i - 1 < n:
            join_pair(slots[i - 1])
        if 0 <= i - 2:
            join_across(slots[i - 2])

    for slot in slots:
        swap_c(slot).wait_recv()
        swap_a(slot).wait_send()
        swap_b(slot).wait_send()
        swap_c(slot).wait_send()
        if slot:
            send_partial(slot).wait_send()
            send_attended(slot).wait_send()


def shards(n, query, key_cache, value_cache, new_key, new_value, lengths, out_weight):
    seqs, q_count, draft, dim = query.shape
    ctx_len, kv_count = key_cache.shape[1:3]
    rows = q_count // 2 * draft
    features, width = out_weight.shape
    span = 2 * ctx_len
    chunk = 4 * PAGE
    half = width // 2
    f32 = jnp.float32
    vmem = pl.BlockSpec(memory_space=pltpu.VMEM)
    anywhere = pl.BlockSpec(memory_space=pl.ANY)
    dma = pltpu.SemaphoreType.DMA
    out = pl.pallas_call(
        functools.partial(kernel, n, draft, chunk),
        out_shape=jax.ShapeDtypeStruct((2, seqs, draft, half), f32),
        in_specs=[
            vmem, anywhere, anywhere, vmem, vmem,
            pl.BlockSpec(memory_space=pltpu.SMEM), anywhere,
        ],
        out_specs=vmem,
        scratch_shapes=[
            pltpu.VMEM((n, span, dim), key_cache.dtype),
            pltpu.VMEM((n, span, dim), value_cache.dtype),
            pltpu.VMEM((2, features, half), out_weight.dtype),
            pltpu.VMEM((span // chunk, rows, chunk), f32),
            pltpu.VMEM((rows, 2 * dim), f32),
            pltpu.VMEM((n - 1, 2 * rows + 8 * (rows // LANES), dim), f32),
            pltpu.VMEM((n - 1, 2 * rows + 8 * (rows // LANES), dim), f32),
            pltpu.VMEM((n, 2 * rows, dim), f32),
        ]
        + [pltpu.VMEM((n, draft, half), f32)] * 5
        + [dma((n,)), dma((n,)), dma((2,))]
        + [dma((n - 1,))] * 4
        + [dma((n,))] * 6,
        compiler_params=pltpu.CompilerParams(
            collective_id=0, has_side_effects=True, vmem_limit_bytes=56 * 2**20
        ),
    )(
        query.reshape(seqs, q_count * draft, dim),
        key_cache.reshape(seqs, span, dim),
        value_cache.reshape(seqs, span, dim),
        new_key, new_value, lengths, out_weight,
    )
    return jnp.transpose(out, (1, 2, 0, 3)).reshape(seqs, draft, width)


def solution(mesh):
    placed = (
        P("groups", "head", None, None),
        P("groups", "ctx", "head", None),
        P("groups", "ctx", "head", None),
        P("groups", "head", None, None),
        P("groups", "head", None, None),
        P("groups"),
        P("head", "ctx"),
    )
    ctx, heads = mesh.shape["ctx"], mesh.shape["head"]

    def body(query, key_cache, *rest):
        fits = (
            query.shape[0] == ctx
            and ctx >= 3
            and heads == 4
            and key_cache.shape[2] == 2
            and query.shape[3] == LANES
            and key_cache.shape[1] % (2 * PAGE) == 0
        )
        if fits:
            return shards(ctx, query, key_cache, *rest)
        return plain_shards(query, key_cache, *rest)

    return jax.shard_map(
        body, mesh=mesh, in_specs=placed, out_specs=P("groups", None, "ctx"), check_vma=False
    )
```

```python
import functools
import math

import jax
import jax.numpy as jnp
from jax import lax
from jax.experimental import pallas as pl
from jax.experimental.pallas import tpu as pltpu
from jax.sharding import PartitionSpec as P

very_low = -1e30
MESH = pl.DeviceIdType.MESH
LANES = 128
PAGE = 256


def plain_shards(query, key_cache, value_cache, new_key, new_value, lengths, out_weight):
    seq_count, q_count, draft_len, head_dim = query.shape
    ctx_len = key_cache.shape[1]
    kv_count = key_cache.shape[2]
    group_rows = q_count // kv_count * draft_len
    scaling = 1.0 / math.sqrt(head_dim)
    grouped = query.reshape(seq_count, kv_count, group_rows, head_dim)
    scores = (
        jnp.einsum("sgrd,stgd->sgrt", grouped, key_cache, preferred_element_type=jnp.float32)
        * scaling
    )
    position = lax.axis_index("ctx") * ctx_len + jnp.arange(ctx_len, dtype=jnp.int32)
    usable = (position[None, :] < lengths[:, None])[:, None, None, :]
    masked = jnp.where(usable, scores, very_low)
    block_top = jnp.max(masked, axis=-1)
    weights = jnp.where(usable, jnp.exp(masked - block_top[..., None]), 0.0).astype(jnp.bfloat16)
    totals = jnp.sum(weights.astype(jnp.float32), axis=-1)
    numerators = jnp.einsum(
        "sgrt,stgd->sgrd", weights, value_cache, preferred_element_type=jnp.float32
    )
    global_top = lax.pmax(block_top, "ctx")
    factor = jnp.exp(block_top - global_top)
    totals, numerators = lax.psum((totals * factor, numerators * factor[..., None]), "ctx")
    own_scores = (
        jnp.einsum("sgrd,sgjd->sgrj", grouped, new_key, preferred_element_type=jnp.float32)
        * scaling
    )
    row_index = jnp.arange(group_rows) % draft_len
    causal = jnp.arange(draft_len)[None, :] <= row_index[:, None]
    own_scores = jnp.where(causal, own_scores, very_low)
    overall = jnp.maximum(global_top, jnp.max(own_scores, axis=-1))
    carried = jnp.exp(global_top - overall)
    fresh_weights = jnp.where(causal, jnp.exp(own_scores - overall[..., None]), 0.0)
    denominator = totals * carried + jnp.sum(fresh_weights, axis=-1)
    numerators = numerators * carried[..., None] + jnp.einsum(
        "sgrj,sgjd->sgrd", fresh_weights, new_value.astype(jnp.float32)
    )
    attended = (numerators / denominator[..., None]).reshape(
        seq_count, q_count, draft_len, head_dim
    )
    attended = (
        jnp.transpose(attended, (0, 2, 1, 3))
        .reshape(seq_count * draft_len, q_count * head_dim)
        .astype(jnp.bfloat16)
    )
    partial_out = jnp.dot(attended, out_weight, preferred_element_type=jnp.float32).reshape(
        seq_count, draft_len, -1
    )
    return lax.psum(partial_out, "head")


def kernel(
    draft, chunk,
    q_ref, k_hbm, v_hbm, nk_ref, nv_ref, len_ref, w_hbm, out_ref,
    kbuf, vbuf, wbuf, sbuf, acc, msg, rmsg, mid, rmid, ag, send_a, keep, recv_a, send_b, recv_b,
    ksem, vsem, wsem, rs_send, rs_recv, mid_send, mid_recv, down_send, down_recv,
    over_send, over_recv, a_send, a_recv, b_send, b_recv, c_send, c_recv,
):
    me = lax.axis_index("ctx")
    head = lax.axis_index("head")
    side = lax.rem(head, 2)
    other = 1 - side
    pair = head - side + other
    upper = lax.rem(lax.div(head, 2), 2)
    across = head + 2 - 4 * upper
    low, high = lax.rem(me, 2), lax.div(me, 2)
    inner = low != high
    outer = low == high
    mate = me + 1 - 2 * low
    facing = 3 - me
    rows = q_ref.shape[1] // 2
    span = kbuf.shape[1]
    half = wbuf.shape[2]
    steps = span // chunk
    blocks = rows // LANES
    scale = math.log2(math.e) / math.sqrt(q_ref.shape[2])

    def seq_of(place):
        return 2 * (high if place % 2 else 1 - high) + place // 2

    barrier = pltpu.get_barrier_semaphore()
    for target in ({"ctx": mate}, {"ctx": facing}, {"head": pair}, {"head": across}):
        pl.semaphore_signal(barrier, inc=1, device_id=target, device_id_type=MESH)

    def k_copy(place):
        return pltpu.make_async_copy(k_hbm.at[seq_of(place)], kbuf.at[place], ksem.at[place])

    def v_copy(place):
        return pltpu.make_async_copy(v_hbm.at[seq_of(place)], vbuf.at[place], vsem.at[place])

    def w_copy(i):
        return pltpu.make_async_copy(w_hbm.at[:, pl.ds(i * half, half)], wbuf.at[i], wsem.at[i])

    for place in range(4):
        k_copy(place).start()
        v_copy(place).start()
    w_copy(0).start()
    w_copy(1).start()

    lane = lax.broadcasted_iota(jnp.int32, (rows, LANES), 1)
    even_lane = lax.rem(lane, 2) == 0
    sub = lax.broadcasted_iota(jnp.int32, (1, 16, LANES), 1)
    even_row = jnp.where(lax.rem(sub, 2) == 0, 1.0, 0.0).astype(jnp.bfloat16)
    odd_row = jnp.where(lax.rem(sub, 2) == 0, 0.0, 1.0).astype(jnp.bfloat16)

    def spread(block):
        tiles = block.reshape(chunk // 16, 16, LANES)
        return jnp.concatenate(
            [(tiles * even_row).reshape(chunk, LANES), (tiles * odd_row).reshape(chunk, LANES)],
            axis=1,
        )

    def pack(ref, top, total):
        stats = jnp.where(lane == 0, top, total).T
        for i in range(blocks):
            ref[rows + 8 * i : rows + 8 * (i + 1), :] = stats[:8, i * LANES : (i + 1) * LANES]

    def unpack(ref):
        packed = jnp.concatenate(
            [ref[rows + 8 * i : rows + 8 * (i + 1), :] for i in range(blocks)], axis=1
        )
        packed = jnp.concatenate([packed, jnp.zeros((LANES - 8, rows), jnp.float32)], axis=0).T
        return packed[:, 0:1], packed[:, 1:2]

    def attend(place):
        s = seq_of(place)
        grouped = jnp.concatenate([q_ref[s, :rows], q_ref[s, rows:]], axis=1)
        usable = len_ref[s] - me * (span // 2)
        k_copy(place).wait()
        per = 2 * PAGE

        def bias(j, page):
            return jnp.where((j * (chunk // per) + page) * PAGE < usable, 0.0, -very_low)

        def score(j, top):
            at = pl.multiple_of(j * chunk, chunk)
            keys = spread(kbuf[place, pl.ds(at, chunk), :])
            scores = lax.dot_general(
                grouped, keys, (((1,), (1,)), ((), ())), preferred_element_type=jnp.float32
            )
            sbuf[j] = scores
            for page in range(chunk // per):
                tiles = [
                    scores[:, page * per + i * LANES : page * per + (i + 1) * LANES]
                    for i in range(per // LANES)
                ]
                top = jnp.maximum(top, functools.reduce(jnp.maximum, tiles) - bias(j, page))
            return top

        top = lax.fori_loop(0, steps, score, jnp.full((rows, LANES), very_low, jnp.float32))
        tops = [
            jnp.max(jnp.where(even_lane, top, very_low), axis=1, keepdims=True) * scale,
            jnp.max(jnp.where(even_lane, very_low, top), axis=1, keepdims=True) * scale,
        ]
        shift = jnp.where(even_lane, tops[0], tops[1])
        v_copy(place).wait()
        acc[...] = jnp.zeros_like(acc)

        def weigh(j, total):
            at = pl.multiple_of(j * chunk, chunk)
            pieces = []
            for page in range(chunk // per):
                shifted = shift + bias(j, page)
                for i in range(per // LANES):
                    piece = jnp.exp2(
                        sbuf[j, :, page * per + i * LANES : page * per + (i + 1) * LANES] * scale
                        - shifted
                    )
                    total = total + piece
                    pieces.append(piece.astype(jnp.bfloat16))
            weights = jnp.concatenate(pieces, axis=1)
            values = spread(vbuf[place, pl.ds(at, chunk), :])
            acc[...] += jnp.dot(weights, values, preferred_element_type=jnp.float32)
            return total

        total = lax.fori_loop(0, steps, weigh, jnp.zeros((rows, LANES), jnp.float32))
        sums = [
            jnp.sum(jnp.where(even_lane, total, 0.0), axis=1, keepdims=True),
            jnp.sum(jnp.where(even_lane, 0.0, total), axis=1, keepdims=True),
        ]
        for g in range(2):
            ref = msg.at[place, g]
            ref[:rows, :] = acc[:, g * LANES : (g + 1) * LANES]
            pack(ref, tops[g], sums[g])

    def remote(source, target, send, recv, axis, device):
        return pltpu.make_async_remote_copy(
            src_ref=source, dst_ref=target, send_sem=send, recv_sem=recv,
            device_id={axis: device}, device_id_type=MESH,
        )

    def inward(p, g):
        return remote(
            msg.at[p, g], rmsg.at[p, g], rs_send.at[p, g], rs_recv.at[p, g], "ctx", mate
        )

    def through(i, g):
        return remote(
            mid.at[i, g], rmid.at[i, g], mid_send.at[i, g], mid_recv.at[i, g], "ctx", facing
        )

    def outward(p, g):
        return remote(
            ag.at[p, g], ag.at[p, g], down_send.at[p, g], down_recv.at[p, g], "ctx", mate
        )

    def over(i, g):
        return remote(
            ag.at[2 * i + 1, g], ag.at[2 * i, g],
            over_send.at[i, g], over_recv.at[i, g], "ctx", facing,
        )

    def join(parts, overall, total, numerator):
        for ref, (top, amount) in parts:
            carried = jnp.exp2(top - overall)
            total = total + amount * carried
            numerator = numerator + ref[:rows, :] * carried
        return total, numerator

    def send_inward(place):
        @pl.when(outer)
        def _():
            for g in range(2):
                inward(place, g).start()

    def merge(i):
        @pl.when(inner)
        def _():
            for g in range(2):
                inward(2 * i, g).wait_recv()
                parts = [(r, unpack(r)) for r in (msg.at[2 * i, g], rmsg.at[2 * i, g])]
                overall = jnp.maximum(parts[0][1][0], parts[1][1][0])
                total, numerator = join(parts, overall, 0.0, 0.0)
                mid[i, g, :rows, :] = numerator
                pack(mid.at[i, g], overall, total)
                through(i, g).start()

    row_in = lax.rem(lax.broadcasted_iota(jnp.int32, (rows, draft), 0), draft)
    causal = lax.broadcasted_iota(jnp.int32, (rows, draft), 1) <= row_in

    def finish(i):
        @pl.when(inner)
        def _():
            place = 2 * i + 1
            s = seq_of(place)
            for g in range(2):
                fresh = lax.dot_general(
                    q_ref[s, g * rows : (g + 1) * rows], nk_ref[s, g],
                    (((1,), (1,)), ((), ())), preferred_element_type=jnp.float32,
                ) * scale
                fresh = jnp.where(causal, fresh, very_low)
                overall = jnp.max(fresh, axis=1, keepdims=True)
                through(i, g).wait_recv()
                inward(place, g).wait_recv()
                refs = (msg.at[place, g], rmsg.at[place, g], rmid.at[i, g])
                parts = [(r, unpack(r)) for r in refs]
                for _, (top, _) in parts:
                    overall = jnp.maximum(overall, top)
                fresh = jnp.where(causal, jnp.exp2(fresh - overall), 0.0)
                total, numerator = join(
                    parts, overall,
                    jnp.sum(fresh, axis=1, keepdims=True),
                    jnp.dot(
                        fresh.astype(jnp.bfloat16), nv_ref[s, g],
                        preferred_element_type=jnp.float32,
                    ),
                )
                ag[place, g] = numerator / total
                over(i, g).start()
                outward(place, g).start()

    def arrive(place):
        @pl.when(outer)
        def _():
            for g in range(2):
                outward(place, g).wait_recv()

        if place % 2 == 0:
            @pl.when(inner)
            def _():
                for g in range(2):
                    over(place // 2, g).wait_recv()
                    outward(place, g).start()

    def swap_a(p):
        return remote(send_a.at[p], recv_a.at[p], a_send.at[p], a_recv.at[p], "head", pair)

    def swap_b(p):
        return remote(send_b.at[p], recv_b.at[p], b_send.at[p], b_recv.at[p], "head", across)

    def swap_c(p):
        part = out_ref.at[side, seq_of(p)]
        return remote(part, part, c_send.at[p], c_recv.at[p], "head", pair)

    wide = 2 * LANES

    def project(place):
        attended = jnp.concatenate(
            [
                ag[place, g, h * draft : (h + 1) * draft, :].astype(jnp.bfloat16)
                for g in range(2)
                for h in range(rows // draft)
            ],
            axis=1,
        )
        for target, which in ((send_a, other), (keep, side)):
            @pl.loop(0, half // wide)
            def _(i):
                at = pl.ds(pl.multiple_of(i * wide, wide), wide)
                target[place, :, at] = jnp.dot(
                    attended, wbuf[which, :, at], preferred_element_type=jnp.float32
                )
            if target is send_a:
                swap_a(place).start()

    def join_pair(place):
        swap_a(place).wait_recv()
        send_b[place] = keep[place] + recv_a[place]
        swap_b(place).start()

    def join_across(place):
        swap_b(place).wait_recv()
        out_ref[side, seq_of(place)] = send_b[place] + recv_b[place]
        swap_c(place).start()

    attend(0)
    pl.semaphore_wait(barrier, 4)
    send_inward(0)
    attend(1)
    send_inward(1)
    merge(0)
    attend(2)
    send_inward(2)
    attend(3)
    send_inward(3)
    w_copy(0).wait()
    w_copy(1).wait()
    finish(0)
    arrive(1)
    project(1)
    merge(1)
    arrive(0)
    project(0)
    join_pair(1)
    finish(1)
    arrive(3)
    project(3)
    join_pair(0)
    join_across(1)
    arrive(2)
    project(2)
    join_pair(3)
    join_across(0)
    join_pair(2)
    join_across(3)
    join_across(2)

    for place in range(4):
        swap_c(place).wait_recv()
        swap_a(place).wait_send()
        swap_b(place).wait_send()
        swap_c(place).wait_send()

    @pl.when(outer)
    def _():
        for place in range(4):
            for g in range(2):
                inward(place, g).wait_send()

    @pl.when(inner)
    def _():
        for g in range(2):
            for place in range(4):
                outward(place, g).wait_send()
            for i in range(2):
                through(i, g).wait_send()
                over(i, g).wait_send()


def shards(n, query, key_cache, value_cache, new_key, new_value, lengths, out_weight):
    seqs, q_count, draft, dim = query.shape
    ctx_len, kv_count = key_cache.shape[1:3]
    rows = q_count // 2 * draft
    features, width = out_weight.shape
    span = 2 * ctx_len
    chunk = 8 * PAGE
    half = width // 2
    message = rows + 8 * (rows // LANES)
    f32 = jnp.float32
    vmem = pl.BlockSpec(memory_space=pltpu.VMEM)
    anywhere = pl.BlockSpec(memory_space=pl.ANY)
    dma = pltpu.SemaphoreType.DMA
    out = pl.pallas_call(
        functools.partial(kernel, draft, chunk),
        out_shape=jax.ShapeDtypeStruct((2, seqs, draft, half), f32),
        in_specs=[
            vmem, anywhere, anywhere, vmem, vmem,
            pl.BlockSpec(memory_space=pltpu.SMEM), anywhere,
        ],
        out_specs=vmem,
        scratch_shapes=[
            pltpu.VMEM((n, span, dim), key_cache.dtype),
            pltpu.VMEM((n, span, dim), value_cache.dtype),
            pltpu.VMEM((2, features, half), out_weight.dtype),
            pltpu.VMEM((span // chunk, rows, chunk), f32),
            pltpu.VMEM((rows, 2 * dim), f32),
            pltpu.VMEM((n, 2, message, dim), f32),
            pltpu.VMEM((n, 2, message, dim), f32),
            pltpu.VMEM((n // 2, 2, message, dim), f32),
            pltpu.VMEM((n // 2, 2, message, dim), f32),
            pltpu.VMEM((n, 2, rows, dim), f32),
        ]
        + [pltpu.VMEM((n, draft, half), f32)] * 5
        + [dma((n,)), dma((n,)), dma((2,))]
        + [dma((n, 2))] * 2
        + [dma((n // 2, 2))] * 2
        + [dma((n, 2))] * 2
        + [dma((n // 2, 2))] * 2
        + [dma((n,))] * 6,
        compiler_params=pltpu.CompilerParams(
            collective_id=0, has_side_effects=True, vmem_limit_bytes=56 * 2**20
        ),
    )(
        query.reshape(seqs, q_count * draft, dim),
        key_cache.reshape(seqs, span, dim),
        value_cache.reshape(seqs, span, dim),
        new_key, new_value, lengths, out_weight,
    )
    return jnp.transpose(out, (1, 2, 0, 3)).reshape(seqs, draft, width)


def solution(mesh):
    placed = (
        P("groups", "head", None, None),
        P("groups", "ctx", "head", None),
        P("groups", "ctx", "head", None),
        P("groups", "head", None, None),
        P("groups", "head", None, None),
        P("groups"),
        P("head", "ctx"),
    )
    ctx, heads = mesh.shape["ctx"], mesh.shape["head"]

    def body(query, key_cache, *rest):
        fits = (
            query.shape[0] == ctx
            and ctx == 4
            and heads == 4
            and key_cache.shape[2] == 2
            and query.shape[3] == LANES
            and key_cache.shape[1] % (4 * PAGE) == 0
        )
        if fits:
            return shards(ctx, query, key_cache, *rest)
        return plain_shards(query, key_cache, *rest)

    return jax.shard_map(
        body, mesh=mesh, in_specs=placed, out_specs=P("groups", None, "ctx"), check_vma=False
    )
```

```python
import functools
import math

import jax
import jax.numpy as jnp
from jax import lax
from jax.experimental import pallas as pl
from jax.experimental.pallas import tpu as pltpu
from jax.sharding import PartitionSpec as P

very_low = -1e30
MESH = pl.DeviceIdType.MESH
LANES = 128
PAGE = 256


def plain_shards(query, key_cache, value_cache, new_key, new_value, lengths, out_weight):
    seq_count, q_count, draft_len, head_dim = query.shape
    ctx_len = key_cache.shape[1]
    kv_count = key_cache.shape[2]
    group_rows = q_count // kv_count * draft_len
    scaling = 1.0 / math.sqrt(head_dim)
    grouped = query.reshape(seq_count, kv_count, group_rows, head_dim)
    scores = (
        jnp.einsum("sgrd,stgd->sgrt", grouped, key_cache, preferred_element_type=jnp.float32)
        * scaling
    )
    position = lax.axis_index("ctx") * ctx_len + jnp.arange(ctx_len, dtype=jnp.int32)
    usable = (position[None, :] < lengths[:, None])[:, None, None, :]
    masked = jnp.where(usable, scores, very_low)
    block_top = jnp.max(masked, axis=-1)
    weights = jnp.where(usable, jnp.exp(masked - block_top[..., None]), 0.0).astype(jnp.bfloat16)
    totals = jnp.sum(weights.astype(jnp.float32), axis=-1)
    numerators = jnp.einsum(
        "sgrt,stgd->sgrd", weights, value_cache, preferred_element_type=jnp.float32
    )
    global_top = lax.pmax(block_top, "ctx")
    factor = jnp.exp(block_top - global_top)
    totals, numerators = lax.psum((totals * factor, numerators * factor[..., None]), "ctx")
    own_scores = (
        jnp.einsum("sgrd,sgjd->sgrj", grouped, new_key, preferred_element_type=jnp.float32)
        * scaling
    )
    row_index = jnp.arange(group_rows) % draft_len
    causal = jnp.arange(draft_len)[None, :] <= row_index[:, None]
    own_scores = jnp.where(causal, own_scores, very_low)
    overall = jnp.maximum(global_top, jnp.max(own_scores, axis=-1))
    carried = jnp.exp(global_top - overall)
    fresh_weights = jnp.where(causal, jnp.exp(own_scores - overall[..., None]), 0.0)
    denominator = totals * carried + jnp.sum(fresh_weights, axis=-1)
    numerators = numerators * carried[..., None] + jnp.einsum(
        "sgrj,sgjd->sgrd", fresh_weights, new_value.astype(jnp.float32)
    )
    attended = (numerators / denominator[..., None]).reshape(
        seq_count, q_count, draft_len, head_dim
    )
    attended = (
        jnp.transpose(attended, (0, 2, 1, 3))
        .reshape(seq_count * draft_len, q_count * head_dim)
        .astype(jnp.bfloat16)
    )
    partial_out = jnp.dot(attended, out_weight, preferred_element_type=jnp.float32).reshape(
        seq_count, draft_len, -1
    )
    return lax.psum(partial_out, "head")


def kernel(
    draft, chunk,
    q_ref, k_hbm, v_hbm, nk_ref, nv_ref, len_ref, w_hbm, out_ref,
    kbuf, vbuf, wbuf, sbuf, acc, msg, rmsg, mid, rmid, ag, send_a, keep, recv_a, send_b, recv_b,
    ksem, vsem, wsem, rs_send, rs_recv, mid_send, mid_recv, down_send, down_recv,
    over_send, over_recv, a_send, a_recv, b_send, b_recv, c_send, c_recv,
):
    me = lax.axis_index("ctx")
    head = lax.axis_index("head")
    side = lax.rem(head, 2)
    other = 1 - side
    pair = head - side + other
    upper = lax.rem(lax.div(head, 2), 2)
    across = head + 2 - 4 * upper
    low, high = lax.rem(me, 2), lax.div(me, 2)
    inner = low != high
    outer = low == high
    mate = me + 1 - 2 * low
    facing = 3 - me
    rows = q_ref.shape[1] // 2
    span = kbuf.shape[1]
    half = wbuf.shape[2]
    steps = span // chunk
    blocks = rows // LANES
    scale = math.log2(math.e) / math.sqrt(q_ref.shape[2])

    def seq_of(place):
        return 2 * (high if place % 2 else 1 - high) + place // 2

    barrier = pltpu.get_barrier_semaphore()
    for target in ({"ctx": mate}, {"ctx": facing}, {"head": pair}, {"head": across}):
        pl.semaphore_signal(barrier, inc=1, device_id=target, device_id_type=MESH)

    def k_copy(place):
        return pltpu.make_async_copy(k_hbm.at[seq_of(place)], kbuf.at[place], ksem.at[place])

    def v_copy(place):
        return pltpu.make_async_copy(v_hbm.at[seq_of(place)], vbuf.at[place], vsem.at[place])

    def w_copy(i):
        return pltpu.make_async_copy(w_hbm.at[:, pl.ds(i * half, half)], wbuf.at[i], wsem.at[i])

    for place in range(4):
        k_copy(place).start()
        v_copy(place).start()
    w_copy(0).start()
    w_copy(1).start()

    lane = lax.broadcasted_iota(jnp.int32, (rows, LANES), 1)
    even_lane = lax.rem(lane, 2) == 0
    sub = lax.broadcasted_iota(jnp.int32, (1, 16, LANES), 1)
    even_row = jnp.where(lax.rem(sub, 2) == 0, 1.0, 0.0).astype(jnp.bfloat16)
    odd_row = jnp.where(lax.rem(sub, 2) == 0, 0.0, 1.0).astype(jnp.bfloat16)

    def spread(block):
        tiles = block.reshape(chunk // 16, 16, LANES)
        return jnp.concatenate(
            [(tiles * even_row).reshape(chunk, LANES), (tiles * odd_row).reshape(chunk, LANES)],
            axis=1,
        )

    def pack(ref, top, total):
        stats = jnp.where(lane == 0, top, total).T
        for i in range(blocks):
            ref[rows + 8 * i : rows + 8 * (i + 1), :] = stats[:8, i * LANES : (i + 1) * LANES]

    def unpack(ref):
        packed = jnp.concatenate(
            [ref[rows + 8 * i : rows + 8 * (i + 1), :] for i in range(blocks)], axis=1
        )
        packed = jnp.concatenate([packed, jnp.zeros((LANES - 8, rows), jnp.float32)], axis=0).T
        return packed[:, 0:1], packed[:, 1:2]

    def attend(place):
        s = seq_of(place)
        grouped = jnp.concatenate([q_ref[s, :rows], q_ref[s, rows:]], axis=1)
        usable = len_ref[s] - me * (span // 2)
        k_copy(place).wait()
        per = 2 * PAGE

        def bias(j, page):
            return jnp.where((j * (chunk // per) + page) * PAGE < usable, 0.0, -very_low)

        def score(j, top):
            at = pl.multiple_of(j * chunk, chunk)
            keys = spread(kbuf[place, pl.ds(at, chunk), :])
            scores = lax.dot_general(
                grouped, keys, (((1,), (1,)), ((), ())), preferred_element_type=jnp.float32
            )
            sbuf[j] = scores
            for page in range(chunk // per):
                tiles = [
                    scores[:, page * per + i * LANES : page * per + (i + 1) * LANES]
                    for i in range(per // LANES)
                ]
                top = jnp.maximum(top, functools.reduce(jnp.maximum, tiles) - bias(j, page))
            return top

        top = lax.fori_loop(0, steps, score, jnp.full((rows, LANES), very_low, jnp.float32))
        tops = [
            jnp.max(jnp.where(even_lane, top, very_low), axis=1, keepdims=True) * scale,
            jnp.max(jnp.where(even_lane, very_low, top), axis=1, keepdims=True) * scale,
        ]
        shift = jnp.where(even_lane, tops[0], tops[1])
        v_copy(place).wait()
        acc[...] = jnp.zeros_like(acc)

        def weigh(j, total):
            at = pl.multiple_of(j * chunk, chunk)
            pieces = []
            for page in range(chunk // per):
                shifted = shift + bias(j, page)
                for i in range(per // LANES):
                    piece = jnp.exp2(
                        sbuf[j, :, page * per + i * LANES : page * per + (i + 1) * LANES] * scale
                        - shifted
                    )
                    total = total + piece
                    pieces.append(piece.astype(jnp.bfloat16))
            weights = jnp.concatenate(pieces, axis=1)
            values = spread(vbuf[place, pl.ds(at, chunk), :])
            acc[...] += jnp.dot(weights, values, preferred_element_type=jnp.float32)
            return total

        total = lax.fori_loop(0, steps, weigh, jnp.zeros((rows, LANES), jnp.float32))
        sums = [
            jnp.sum(jnp.where(even_lane, total, 0.0), axis=1, keepdims=True),
            jnp.sum(jnp.where(even_lane, 0.0, total), axis=1, keepdims=True),
        ]
        for g in range(2):
            ref = msg.at[place, g]
            ref[:rows, :] = acc[:, g * LANES : (g + 1) * LANES]
            pack(ref, tops[g], sums[g])

    def remote(source, target, send, recv, axis, device):
        return pltpu.make_async_remote_copy(
            src_ref=source, dst_ref=target, send_sem=send, recv_sem=recv,
            device_id={axis: device}, device_id_type=MESH,
        )

    def inward(p, g):
        return remote(
            msg.at[p, g], rmsg.at[p, g], rs_send.at[p, g], rs_recv.at[p, g], "ctx", mate
        )

    def through(i, g):
        return remote(
            mid.at[i, g], rmid.at[i, g], mid_send.at[i, g], mid_recv.at[i, g], "ctx", facing
        )

    def outward(p, g):
        return remote(
            ag.at[p, g], ag.at[p, g], down_send.at[p, g], down_recv.at[p, g], "ctx", mate
        )

    def over(i, g):
        return remote(
            ag.at[2 * i + 1, g], ag.at[2 * i, g],
            over_send.at[i, g], over_recv.at[i, g], "ctx", facing,
        )

    def join(parts, overall, total, numerator):
        for ref, (top, amount) in parts:
            carried = jnp.exp2(top - overall)
            total = total + amount * carried
            numerator = numerator + ref[:rows, :] * carried
        return total, numerator

    def send_inward(place):
        @pl.when(outer)
        def _():
            for g in range(2):
                inward(place, g).start()

    def merge(i):
        @pl.when(inner)
        def _():
            for g in range(2):
                inward(2 * i, g).wait_recv()
                parts = [(r, unpack(r)) for r in (msg.at[2 * i, g], rmsg.at[2 * i, g])]
                overall = jnp.maximum(parts[0][1][0], parts[1][1][0])
                total, numerator = join(parts, overall, 0.0, 0.0)
                mid[i, g, :rows, :] = numerator
                pack(mid.at[i, g], overall, total)
                through(i, g).start()

    row_in = lax.rem(lax.broadcasted_iota(jnp.int32, (rows, draft), 0), draft)
    causal = lax.broadcasted_iota(jnp.int32, (rows, draft), 1) <= row_in

    def finish(i):
        @pl.when(inner)
        def _():
            place = 2 * i + 1
            s = seq_of(place)
            for g in range(2):
                fresh = lax.dot_general(
                    q_ref[s, g * rows : (g + 1) * rows], nk_ref[s, g],
                    (((1,), (1,)), ((), ())), preferred_element_type=jnp.float32,
                ) * scale
                fresh = jnp.where(causal, fresh, very_low)
                overall = jnp.max(fresh, axis=1, keepdims=True)
                through(i, g).wait_recv()
                inward(place, g).wait_recv()
                refs = (msg.at[place, g], rmsg.at[place, g], rmid.at[i, g])
                parts = [(r, unpack(r)) for r in refs]
                for _, (top, _) in parts:
                    overall = jnp.maximum(overall, top)
                fresh = jnp.where(causal, jnp.exp2(fresh - overall), 0.0)
                total, numerator = join(
                    parts, overall,
                    jnp.sum(fresh, axis=1, keepdims=True),
                    jnp.dot(
                        fresh.astype(jnp.bfloat16), nv_ref[s, g],
                        preferred_element_type=jnp.float32,
                    ),
                )
                ag[place, g] = numerator / total
                over(i, g).start()
                outward(place, g).start()

    def arrive(place):
        @pl.when(outer)
        def _():
            for g in range(2):
                outward(place, g).wait_recv()

    def relay(i):
        @pl.when(inner)
        def _():
            for g in range(2):
                over(i, g).wait_recv()
                outward(2 * i, g).start()

    def swap_a(p):
        return remote(send_a.at[p], recv_a.at[p], a_send.at[p], a_recv.at[p], "head", pair)

    def swap_b(p):
        return remote(send_b.at[p], recv_b.at[p], b_send.at[p], b_recv.at[p], "head", across)

    def swap_c(p):
        part = out_ref.at[side, seq_of(p)]
        return remote(part, part, c_send.at[p], c_recv.at[p], "head", pair)

    wide = 2 * LANES

    def project(place):
        attended = jnp.concatenate(
            [
                ag[place, g, h * draft : (h + 1) * draft, :].astype(jnp.bfloat16)
                for g in range(2)
                for h in range(rows // draft)
            ],
            axis=1,
        )
        for target, which in ((send_a, other), (keep, side)):
            @pl.loop(0, half // wide)
            def _(i):
                at = pl.ds(pl.multiple_of(i * wide, wide), wide)
                target[place, :, at] = jnp.dot(
                    attended, wbuf[which, :, at], preferred_element_type=jnp.float32
                )
            if target is send_a:
                swap_a(place).start()

    def join_pair(place):
        swap_a(place).wait_recv()
        send_b[place] = keep[place] + recv_a[place]
        swap_b(place).start()

    def join_across(place):
        swap_b(place).wait_recv()
        out_ref[side, seq_of(place)] = send_b[place] + recv_b[place]
        swap_c(place).start()

    attend(0)
    pl.semaphore_wait(barrier, 4)
    send_inward(0)
    attend(1)
    send_inward(1)
    merge(0)
    attend(2)
    send_inward(2)
    attend(3)
    send_inward(3)
    w_copy(0).wait()
    w_copy(1).wait()
    finish(0)
    arrive(1)
    project(1)
    merge(1)
    relay(0)
    join_pair(1)
    arrive(0)
    project(0)
    finish(1)
    join_pair(0)
    join_across(1)
    arrive(3)
    project(3)
    relay(1)
    join_pair(3)
    join_across(0)
    arrive(2)
    project(2)
    join_pair(2)
    join_across(3)
    join_across(2)

    for place in range(4):
        swap_c(place).wait_recv()
        swap_a(place).wait_send()
        swap_b(place).wait_send()
        swap_c(place).wait_send()

    @pl.when(outer)
    def _():
        for place in range(4):
            for g in range(2):
                inward(place, g).wait_send()

    @pl.when(inner)
    def _():
        for g in range(2):
            for place in range(4):
                outward(place, g).wait_send()
            for i in range(2):
                through(i, g).wait_send()
                over(i, g).wait_send()


def shards(n, query, key_cache, value_cache, new_key, new_value, lengths, out_weight):
    seqs, q_count, draft, dim = query.shape
    ctx_len, kv_count = key_cache.shape[1:3]
    rows = q_count // 2 * draft
    features, width = out_weight.shape
    span = 2 * ctx_len
    chunk = 8 * PAGE
    half = width // 2
    message = rows + 8 * (rows // LANES)
    f32 = jnp.float32
    vmem = pl.BlockSpec(memory_space=pltpu.VMEM)
    anywhere = pl.BlockSpec(memory_space=pl.ANY)
    dma = pltpu.SemaphoreType.DMA
    out = pl.pallas_call(
        functools.partial(kernel, draft, chunk),
        out_shape=jax.ShapeDtypeStruct((2, seqs, draft, half), f32),
        in_specs=[
            vmem, anywhere, anywhere, vmem, vmem,
            pl.BlockSpec(memory_space=pltpu.SMEM), anywhere,
        ],
        out_specs=vmem,
        scratch_shapes=[
            pltpu.VMEM((n, span, dim), key_cache.dtype),
            pltpu.VMEM((n, span, dim), value_cache.dtype),
            pltpu.VMEM((2, features, half), out_weight.dtype),
            pltpu.VMEM((span // chunk, rows, chunk), f32),
            pltpu.VMEM((rows, 2 * dim), f32),
            pltpu.VMEM((n, 2, message, dim), f32),
            pltpu.VMEM((n, 2, message, dim), f32),
            pltpu.VMEM((n // 2, 2, message, dim), f32),
            pltpu.VMEM((n // 2, 2, message, dim), f32),
            pltpu.VMEM((n, 2, rows, dim), f32),
        ]
        + [pltpu.VMEM((n, draft, half), f32)] * 5
        + [dma((n,)), dma((n,)), dma((2,))]
        + [dma((n, 2))] * 2
        + [dma((n // 2, 2))] * 2
        + [dma((n, 2))] * 2
        + [dma((n // 2, 2))] * 2
        + [dma((n,))] * 6,
        compiler_params=pltpu.CompilerParams(
            collective_id=0, has_side_effects=True, vmem_limit_bytes=56 * 2**20
        ),
    )(
        query.reshape(seqs, q_count * draft, dim),
        key_cache.reshape(seqs, span, dim),
        value_cache.reshape(seqs, span, dim),
        new_key, new_value, lengths, out_weight,
    )
    return jnp.transpose(out, (1, 2, 0, 3)).reshape(seqs, draft, width)


def solution(mesh):
    placed = (
        P("groups", "head", None, None),
        P("groups", "ctx", "head", None),
        P("groups", "ctx", "head", None),
        P("groups", "head", None, None),
        P("groups", "head", None, None),
        P("groups"),
        P("head", "ctx"),
    )
    ctx, heads = mesh.shape["ctx"], mesh.shape["head"]

    def body(query, key_cache, *rest):
        fits = (
            query.shape[0] == ctx
            and ctx == 4
            and heads == 4
            and key_cache.shape[2] == 2
            and query.shape[3] == LANES
            and key_cache.shape[1] % (4 * PAGE) == 0
        )
        if fits:
            return shards(ctx, query, key_cache, *rest)
        return plain_shards(query, key_cache, *rest)

    return jax.shard_map(
        body, mesh=mesh, in_specs=placed, out_specs=P("groups", None, "ctx"), check_vma=False
    )
```
